32 devices in a mesh: depth: 4 (over z), imgx: 4 (over y, core), imgy: 2 (over x).
Axes of the slice: x: 2, y: 2, z: 4, core: 2. Of those that a mesh axis runs over, the one named last changes fastest.
Arguments:
- emissivity: bfloat16 [32, 512, 256], P('depth', 'imgx', 'imgy'), may hold values from 0.099609375 to 10
- bin_index: int32 [32, 512, 256], P('depth', 'imgx', 'imgy'), may hold values from 0 to 127
- color_table: bfloat16 [4, 128], replicated, may hold values from 0.049804688 to 1
- brick_order: int32 [4], replicated, may hold values from 0 to 3, each once
Outputs:
- image: float32 [4, 512, 256], P(None, 'imgx', 'imgy')
The draws below stay inside these ranges and needn't reach their ends.
Inputs may be any that keep to these rules, and one draw needn't show every extreme that they name: brick_order names every brick index once.
All inputs are finite; a program needn't handle non-finite values.
Results may differ from the reference program's by a relative error of at most 0.0003.
Values sent between devices are 32-bit elements; how exact they have to be, the bound alone decides.
No kernel may reach another device: no remote copies, remote signals or barrier semaphores. Data moves between devices by JAX's collectives and lax.ppermute only.
A program may use at most 64 MiB of HBM per device.

```python
import math
import jax
import jax.numpy as jnp
from jax import lax

DZ = 8
BINS = 128
NZ = 32
NX = 512
NY = 256
N_DEPTH = 4


def set_ends(entries, rng, least, high):
    extent = entries.shape
    index_at = [jax.random.randint(jax.random.fold_in(rng, axis), (), 0, extent[axis]) for axis in range(len(extent))]
    entries = entries.at[tuple(index_at)].set(least)
    longest = extent.index(max(extent))
    index_at[longest] = (index_at[longest] + 1) % extent[longest]
    return entries.at[tuple(index_at)].set(high)


def level_of(rng, shape, split, least, largest):
    level = 1.0
    for dim, shards_of in split:
        heights = jax.random.uniform(jax.random.fold_in(jax.random.fold_in(rng, 6), dim), (shards_of,), jnp.float32, least / len(split), largest / len(split))
        level = level * jnp.repeat(jnp.exp(heights), shape[dim] // shards_of).reshape((-1,) + (1,) * (len(shape) - 1 - dim))
    return level


def setup_inputs(seed: int = 0) -> dict:
    keys = jax.random.split(jax.random.key(seed), 5)
    emissivity = jnp.clip(jnp.exp(math.log(10.0) - 4.609084 * jax.random.uniform(keys[0], (NZ, NX, NY), jnp.float32) ** level_of(keys[0], (NZ, NX, NY), ((0, 4), (1, 4), (2, 2)), -0.2, 0.2)), 0.099609375, 10.0).astype(jnp.bfloat16)
    bin_index = set_ends(jax.random.randint(keys[1], (NZ, NX, NY), 0, BINS), jax.random.fold_in(keys[1], 1), 0, BINS - 1).astype(jnp.int32)
    color_table = jnp.clip(jnp.exp(jax.random.uniform(keys[2], (4, BINS), jnp.float32, math.log(0.049804688), math.log(1.0))), 0.049804688, 1.0).astype(jnp.bfloat16)
    brick_order = jax.random.permutation(keys[3], N_DEPTH).astype(jnp.int32)
    return dict(emissivity=emissivity, bin_index=bin_index, color_table=color_table, brick_order=brick_order)


def brick_partial(bright_cells, bin_cells, color_table, ray_step):
    looked = color_table.astype(jnp.float32)[:, bin_cells]
    bright = bright_cells.astype(jnp.float32)
    glow_rgb = bright[None] * looked[0:3]
    absorb_rate = bright * looked[3]
    depth_in = jnp.cumsum(absorb_rate, axis=0) - absorb_rate
    light_in = jnp.exp(-ray_step * depth_in)
    color_sum = jnp.sum(ray_step * glow_rgb * light_in[None], axis=1)
    passed = jnp.exp(-ray_step * jnp.sum(absorb_rate, axis=0))
    return color_sum, passed


def reference(emissivity, bin_index, color_table, brick_order):
    ray_step = 2.0 / NZ

    def advance(state_pair, brick_id):
        color_acc, through = state_pair
        start_cell = (brick_id * DZ).astype(jnp.int32)
        brick_cells = lax.dynamic_slice_in_dim(emissivity, start_cell, DZ, 0)
        brick_bins = lax.dynamic_slice_in_dim(bin_index, start_cell, DZ, 0)
        color_sum, passed = brick_partial(brick_cells, brick_bins, color_table, ray_step)
        return (color_acc + through[None] * color_sum, through * passed), None

    start_state = (jnp.zeros((3, NX, NY), jnp.float32), jnp.ones((NX, NY), jnp.float32))
    final_state, _ = lax.scan(advance, start_state, brick_order)
    color_acc, through = final_state
    return jnp.concatenate([color_acc, (1.0 - through)[None]], 0)
```

```python
import functools
import math

import jax
import jax.numpy as jnp
from jax import lax
from jax.experimental import pallas as pl
from jax.experimental.pallas import tpu as pltpu
from jax.sharding import PartitionSpec as P

LANES = 128
LANE_GATHER = lax.GatherDimensionNumbers(
    offset_dims=(),
    collapsed_slice_dims=(1,),
    start_index_map=(1,),
    operand_batching_dims=(0,),
    start_indices_batching_dims=(0,),
)


def lane_lookup(table, index):
    return lax.gather(
        table,
        index[..., None],
        LANE_GATHER,
        slice_sizes=(1, 1),
        mode=lax.GatherScatterMode.PROMISE_IN_BOUNDS,
    )


def table_lookup(chunks, bins):
    if len(chunks) == 1:
        return lane_lookup(chunks[0], bins)
    low = bins % LANES
    high = bins // LANES
    out = lane_lookup(chunks[0], low)
    for c in range(1, len(chunks)):
        out = jnp.where(high == c, lane_lookup(chunks[c], low), out)
    return out


def load_table(table_ref, rows, rate_scale):
    channels, bins = table_ref.shape
    table = table_ref[...].astype(jnp.float32)
    chunks = []
    for ch in range(channels):
        row = table[ch : ch + 1, :]
        if ch == channels - 1:
            row = row * rate_scale
        chunks.append(
            [jnp.broadcast_to(row[:, c : c + LANES], (rows, LANES)) for c in range(0, bins, LANES)]
        )
    return chunks


def block_partial(emis_ref, bins_ref, chunks, row, rows, col, ray_step):
    depth_cells = emis_ref.shape[0]
    color = [None] * 3
    depth_sum = None
    for k in range(depth_cells):
        bright = emis_ref[k, pl.ds(row, rows), col : col + LANES].astype(jnp.float32)
        bins = bins_ref[k, pl.ds(row, rows), col : col + LANES]
        rate = bright * table_lookup(chunks[3], bins)
        if k:
            bright = bright * jnp.exp2(depth_sum)
        depth_sum = rate if depth_sum is None else depth_sum + rate
        for ch in range(3):
            term = bright * table_lookup(chunks[ch], bins)
            color[ch] = term if color[ch] is None else color[ch] + term
    return [c * ray_step for c in color] + [jnp.exp2(depth_sum)]


def partial_kernel(emis_ref, bins_ref, table_ref, *out_refs, ray_step, rows):
    me = lax.axis_index("depth")
    piece_rows, cols = out_refs[0].shape[1:]
    chunks = load_table(table_ref, rows, -ray_step * math.log2(math.e))
    for s, out_ref in enumerate(out_refs):
        first = (me ^ s) * piece_rows
        for r in range(0, piece_rows, rows):
            for col in range(0, cols, LANES):
                row = pl.multiple_of(first + r, rows)
                planes = block_partial(emis_ref, bins_ref, chunks, row, rows, col, ray_step)
                for ch, plane in enumerate(planes):
                    out_ref[ch, r : r + rows, col : col + LANES] = plane


def composite_kernel(order_ref, *refs):
    me = lax.axis_index("depth")
    in_refs, out_ref = refs[:-1], refs[-1]
    n = len(in_refs)

    def pick(slot, ch):
        value = in_refs[0][ch]
        for s in range(1, n):
            value = jnp.where(slot == s, in_refs[s][ch], value)
        return value

    color = [None] * 3
    through = None
    for k in range(n):
        slot = me ^ order_ref[k]
        for ch in range(3):
            term = pick(slot, ch)
            if k:
                term = color[ch] + through * term
            color[ch] = term
        passed = pick(slot, 3)
        through = passed if through is None else through * passed
    for ch in range(3):
        out_ref[ch] = color[ch]
    out_ref[3] = 1.0 - through


def assemble_kernel(*refs):
    me = lax.axis_index("depth")
    in_refs, out_ref = refs[:-1], refs[-1]
    piece_rows = in_refs[0].shape[1]
    for s, in_ref in enumerate(in_refs):
        row = pl.multiple_of((me ^ s) * piece_rows, piece_rows)
        out_ref[:, pl.ds(row, piece_rows), :] = in_ref[...]


def exchange(pieces, devices):
    received = [None] * devices
    for s in reversed(range(1, devices)):
        received[s] = lax.ppermute(pieces[s], "depth", [(d, d ^ s) for d in range(devices)])
    return received


VMEM = pl.BlockSpec(memory_space=pltpu.VMEM)
SMEM = pl.BlockSpec(memory_space=pltpu.SMEM)


def by_exchange(emissivity, bin_index, color_table, brick_order, devices, ray_step):
    depth_cells, cols_x, cols_y = emissivity.shape
    piece_rows = cols_x // devices
    rows = 16 if piece_rows % 16 == 0 else 8
    piece = jax.ShapeDtypeStruct((4, piece_rows, cols_y), jnp.float32)
    pieces = pl.pallas_call(
        functools.partial(partial_kernel, ray_step=ray_step, rows=rows),
        out_shape=[piece] * devices,
        in_specs=[VMEM, VMEM, VMEM],
        out_specs=[VMEM] * devices,
        name="partial",
    )(emissivity, bin_index, color_table)
    received = exchange(pieces, devices)
    received[0] = pieces[0]
    mine = pl.pallas_call(
        composite_kernel,
        out_shape=piece,
        in_specs=[SMEM] + [VMEM] * devices,
        out_specs=VMEM,
        name="composite",
    )(brick_order, *received)
    tiles = exchange([mine] * devices, devices)
    tiles[0] = mine
    return pl.pallas_call(
        assemble_kernel,
        out_shape=jax.ShapeDtypeStruct((4, cols_x, cols_y), jnp.float32),
        in_specs=[VMEM] * devices,
        out_specs=VMEM,
        name="assemble",
    )(*tiles)


def whole_partial_kernel(emis_ref, bins_ref, table_ref, out_ref, *, ray_step, rows):
    chunks = load_table(table_ref, rows, -ray_step * math.log2(math.e))
    cols_x, cols_y = out_ref.shape[1:]

    def step(b, carry):
        row = pl.multiple_of(b * rows, rows)
        for col in range(0, cols_y, LANES):
            planes = block_partial(emis_ref, bins_ref, chunks, row, rows, col, ray_step)
            for ch, plane in enumerate(planes):
                out_ref[ch, pl.ds(row, rows), col : col + LANES] = plane
        return carry

    lax.fori_loop(0, cols_x // rows, step, 0)


def by_collectives(emissivity, bin_index, color_table, brick_order, devices, ray_step):
    depth_cells, cols_x, cols_y = emissivity.shape
    partials = pl.pallas_call(
        functools.partial(whole_partial_kernel, ray_step=ray_step, rows=8),
        out_shape=jax.ShapeDtypeStruct((4, cols_x, cols_y), jnp.float32),
        in_specs=[VMEM, VMEM, VMEM],
        out_specs=VMEM,
        name="partial_whole",
    )(emissivity, bin_index, color_table)
    pieces = partials.reshape(4, devices, cols_x // devices, cols_y).transpose(1, 0, 2, 3)
    received = lax.all_to_all(pieces, "depth", split_axis=0, concat_axis=0, tiled=True)

    def advance(state, brick):
        color, through = state
        planes = lax.dynamic_index_in_dim(received, brick, 0, keepdims=False)
        return (color + through * planes[0:3], through * planes[3]), None

    start = (jnp.zeros_like(received[0, 0:3]), jnp.ones_like(received[0, 3]))
    (color, through), _ = lax.scan(advance, start, brick_order)
    mine = jnp.concatenate([color, (1.0 - through)[None]], 0)
    return lax.all_gather(mine, "depth", axis=1, tiled=True)


def on_device(emissivity, bin_index, color_table, brick_order):
    depth_cells, cols_x, cols_y = emissivity.shape
    devices = lax.axis_size("depth")
    ray_step = 2.0 / (depth_cells * devices)
    few = devices <= 8 and devices & (devices - 1) == 0 and cols_x % (8 * devices) == 0
    plan = by_exchange if few else by_collectives
    return plan(emissivity, bin_index, color_table, brick_order, devices, ray_step)


def solution(mesh):
    return jax.shard_map(
        on_device,
        mesh=mesh,
        in_specs=(P("depth", "imgx", "imgy"), P("depth", "imgx", "imgy"), P(), P()),
        out_specs=P(None, "imgx", "imgy"),
        check_vma=False,
    )
```

```python
import functools
import math

import jax
import jax.numpy as jnp
from jax import lax
from jax.experimental import pallas as pl
from jax.experimental.pallas import tpu as pltpu
from jax.sharding import PartitionSpec as P

LANES = 128
LANE_GATHER = lax.GatherDimensionNumbers(
    offset_dims=(),
    collapsed_slice_dims=(1,),
    start_index_map=(1,),
    operand_batching_dims=(0,),
    start_indices_batching_dims=(0,),
)


def lane_lookup(table, index):
    return lax.gather(
        table,
        index[..., None],
        LANE_GATHER,
        slice_sizes=(1, 1),
        mode=lax.GatherScatterMode.PROMISE_IN_BOUNDS,
    )


def table_lookup(chunks, bins):
    if len(chunks) == 1:
        return lane_lookup(chunks[0], bins)
    low = bins % LANES
    high = bins // LANES
    out = lane_lookup(chunks[0], low)
    for c in range(1, len(chunks)):
        out = jnp.where(high == c, lane_lookup(chunks[c], low), out)
    return out


def load_table(table_ref, rows, rate_scale):
    channels, bins = table_ref.shape
    table = table_ref[...].astype(jnp.float32)
    chunks = []
    for ch in range(channels):
        row = table[ch : ch + 1, :]
        if ch == channels - 1:
            row = row * rate_scale
        chunks.append(
            [jnp.broadcast_to(row[:, c : c + LANES], (rows, LANES)) for c in range(0, bins, LANES)]
        )
    return chunks


def block_partial(emis_ref, bins_ref, chunks, row, rows, col, ray_step):
    depth_cells = emis_ref.shape[0]
    color = [None] * 3
    depth_sum = None
    for k in range(depth_cells):
        bright = emis_ref[k, pl.ds(row, rows), col : col + LANES].astype(jnp.float32)
        bins = bins_ref[k, pl.ds(row, rows), col : col + LANES]
        rate = bright * table_lookup(chunks[3], bins)
        if k:
            bright = bright * jnp.exp2(depth_sum)
        depth_sum = rate if depth_sum is None else depth_sum + rate
        for ch in range(3):
            term = bright * table_lookup(chunks[ch], bins)
            color[ch] = term if color[ch] is None else color[ch] + term
    return [c * ray_step for c in color] + [jnp.exp2(depth_sum)]


def partial_kernel(emis_ref, bins_ref, table_ref, *out_refs, ray_step, rows):
    me = lax.axis_index("depth")
    piece_rows, cols = out_refs[0].shape[1:]
    chunks = load_table(table_ref, rows, -ray_step * math.log2(math.e))
    for s, out_ref in enumerate(out_refs):
        first = (me ^ s) * piece_rows
        for r in range(0, piece_rows, rows):
            for col in range(0, cols, LANES):
                row = pl.multiple_of(first + r, rows)
                planes = block_partial(emis_ref, bins_ref, chunks, row, rows, col, ray_step)
                for ch, plane in enumerate(planes):
                    out_ref[ch, r : r + rows, col : col + LANES] = plane


def composite_kernel(order_ref, *refs):
    me = lax.axis_index("depth")
    in_refs, out_ref = refs[:-1], refs[-1]
    n = len(in_refs)

    def pick(slot, ch):
        value = in_refs[0][ch]
        for s in range(1, n):
            value = jnp.where(slot == s, in_refs[s][ch], value)
        return value

    color = [None] * 3
    through = None
    for k in range(n):
        slot = me ^ order_ref[k]
        for ch in range(3):
            term = pick(slot, ch)
            if k:
                term = color[ch] + through * term
            color[ch] = term
        passed = pick(slot, 3)
        through = passed if through is None else through * passed
    for ch in range(3):
        out_ref[ch] = color[ch]
    out_ref[3] = 1.0 - through


def assemble_kernel(*refs):
    me = lax.axis_index("depth")
    in_refs, out_ref, sems = refs[:-2], refs[-2], refs[-1]
    piece_rows = in_refs[0].shape[1]
    copies = []
    for s, in_ref in enumerate(in_refs):
        row = pl.multiple_of((me ^ s) * piece_rows, piece_rows)
        copies.append(
            pltpu.make_async_copy(in_ref, out_ref.at[:, pl.ds(row, piece_rows), :], sems.at[s])
        )
    for copy in copies:
        copy.start()
    for copy in copies:
        copy.wait()


def exchange(pieces, devices):
    received = [None] * devices
    for s in reversed(range(1, devices)):
        received[s] = lax.ppermute(pieces[s], "depth", [(d, d ^ s) for d in range(devices)])
    return received


VMEM = pl.BlockSpec(memory_space=pltpu.VMEM)
SMEM = pl.BlockSpec(memory_space=pltpu.SMEM)
ANY = pl.BlockSpec(memory_space=pl.ANY)


def in_vmem(arrays):
    return [pltpu.with_memory_space_constraint(a, pltpu.VMEM) for a in arrays]


def by_exchange(emissivity, bin_index, color_table, brick_order, devices, ray_step):
    depth_cells, cols_x, cols_y = emissivity.shape
    piece_rows = cols_x // devices
    rows = 16 if piece_rows % 16 == 0 else 8
    piece = pltpu.VMEM((4, piece_rows, cols_y), jnp.float32)
    pieces = pl.pallas_call(
        functools.partial(partial_kernel, ray_step=ray_step, rows=rows),
        out_shape=[piece] * devices,
        in_specs=[VMEM, VMEM, VMEM],
        out_specs=[VMEM] * devices,
        name="partial",
    )(emissivity, bin_index, color_table)
    received = exchange(pieces, devices)
    received[0] = pieces[0]
    mine = pl.pallas_call(
        composite_kernel,
        out_shape=piece,
        in_specs=[SMEM] + [VMEM] * devices,
        out_specs=VMEM,
        name="composite",
    )(brick_order, *in_vmem(received))
    tiles = exchange([mine] * devices, devices)
    tiles[0] = mine
    return pl.pallas_call(
        assemble_kernel,
        out_shape=jax.ShapeDtypeStruct((4, cols_x, cols_y), jnp.float32),
        in_specs=[VMEM] * devices,
        out_specs=ANY,
        scratch_shapes=[pltpu.SemaphoreType.DMA((devices,))],
        name="assemble",
    )(*in_vmem(tiles))


def whole_partial_kernel(emis_ref, bins_ref, table_ref, out_ref, *, ray_step, rows):
    chunks = load_table(table_ref, rows, -ray_step * math.log2(math.e))
    cols_x, cols_y = out_ref.shape[1:]

    def step(b, carry):
        row = pl.multiple_of(b * rows, rows)
        for col in range(0, cols_y, LANES):
            planes = block_partial(emis_ref, bins_ref, chunks, row, rows, col, ray_step)
            for ch, plane in enumerate(planes):
                out_ref[ch, pl.ds(row, rows), col : col + LANES] = plane
        return carry

    lax.fori_loop(0, cols_x // rows, step, 0)


def by_collectives(emissivity, bin_index, color_table, brick_order, devices, ray_step):
    depth_cells, cols_x, cols_y = emissivity.shape
    partials = pl.pallas_call(
        functools.partial(whole_partial_kernel, ray_step=ray_step, rows=8),
        out_shape=jax.ShapeDtypeStruct((4, cols_x, cols_y), jnp.float32),
        in_specs=[VMEM, VMEM, VMEM],
        out_specs=VMEM,
        name="partial_whole",
    )(emissivity, bin_index, color_table)
    pieces = partials.reshape(4, devices, cols_x // devices, cols_y).transpose(1, 0, 2, 3)
    received = lax.all_to_all(pieces, "depth", split_axis=0, concat_axis=0, tiled=True)

    def advance(state, brick):
        color, through = state
        planes = lax.dynamic_index_in_dim(received, brick, 0, keepdims=False)
        return (color + through * planes[0:3], through * planes[3]), None

    start = (jnp.zeros_like(received[0, 0:3]), jnp.ones_like(received[0, 3]))
    (color, through), _ = lax.scan(advance, start, brick_order)
    mine = jnp.concatenate([color, (1.0 - through)[None]], 0)
    return lax.all_gather(mine, "depth", axis=1, tiled=True)


def on_device(emissivity, bin_index, color_table, brick_order):
    depth_cells, cols_x, cols_y = emissivity.shape
    devices = lax.axis_size("depth")
    ray_step = 2.0 / (depth_cells * devices)
    few = devices <= 8 and devices & (devices - 1) == 0 and cols_x % (8 * devices) == 0
    plan = by_exchange if few else by_collectives
    return plan(emissivity, bin_index, color_table, brick_order, devices, ray_step)


def solution(mesh):
    return jax.shard_map(
        on_device,
        mesh=mesh,
        in_specs=(P("depth", "imgx", "imgy"), P("depth", "imgx", "imgy"), P(), P()),
        out_specs=P(None, "imgx", "imgy"),
        check_vma=False,
    )
```

```python
import functools
import math

import jax
import jax.numpy as jnp
from jax import lax
from jax.experimental import pallas as pl
from jax.experimental.pallas import tpu as pltpu
from jax.sharding import PartitionSpec as P


LANES = 128
TABLE_STEPS = 4096.0
FIELD_BITS = 13
FIELD = 1 << FIELD_BITS
ROWS = 8
READY = (3,)
OUT_ORDER = ((1, 3, 0, 2), (3, 2, 1, 0), (2, 0, 3, 1))
BACK_ORDER = ((1, 2, 3, 0), (2, 3, 0, 1), (3, 0, 1, 2))
LANE_GATHER = lax.GatherDimensionNumbers(
    offset_dims=(),
    collapsed_slice_dims=(1,),
    start_index_map=(1,),
    operand_batching_dims=(0,),
    start_indices_batching_dims=(0,),
)


def lane_lookup(table, index):
    return lax.gather(
        table,
        index[..., None],
        LANE_GATHER,
        slice_sizes=(1, 1),
        mode=lax.GatherScatterMode.PROMISE_IN_BOUNDS,
    )


def load_table(table_ref, rows):
    channels, bins = table_ref.shape
    table = table_ref[...].astype(jnp.float32)
    steps = (table * TABLE_STEPS).astype(jnp.int32)
    packed = []
    for ch in range(0, channels, 2):
        row = steps[ch : ch + 1, :] * FIELD + steps[ch + 1 : ch + 2, :]
        packed.append(
            [jnp.broadcast_to(row[:, c : c + LANES], (rows, LANES)) for c in range(0, bins, LANES)]
        )
    return packed


def table_lookup(chunks, bins):
    if len(chunks) == 1:
        both = lane_lookup(chunks[0], bins)
    else:
        low = bins % LANES
        high = bins // LANES
        both = lane_lookup(chunks[0], low)
        for c in range(1, len(chunks)):
            both = jnp.where(high == c, lane_lookup(chunks[c], low), both)
    first = lax.shift_right_logical(both, FIELD_BITS)
    second = both & (FIELD - 1)
    return first.astype(jnp.float32), second.astype(jnp.float32)


def block_partial(cells, packed, depth_cells, ray_step):
    rate_scale = -ray_step * math.log2(math.e) / TABLE_STEPS
    color = [None] * 3
    depth_sum = None
    for k in range(depth_cells):
        bright, bins = cells(k)
        bright = bright.astype(jnp.float32)
        red, green = table_lookup(packed[0], bins)
        blue, absorb = table_lookup(packed[1], bins)
        rate = bright * absorb
        if k:
            bright = bright * jnp.exp2(depth_sum * rate_scale)
        depth_sum = rate if depth_sum is None else depth_sum + rate
        for ch, factor in enumerate((red, green, blue)):
            term = bright * factor
            color[ch] = term if color[ch] is None else color[ch] + term
    scale = ray_step / TABLE_STEPS
    return [c * scale for c in color] + [jnp.exp2(depth_sum * rate_scale)]


def lookup(table, me):
    value = jnp.int32(table[0])
    for d in range(1, len(table)):
        value = jnp.where(me == d, jnp.int32(table[d]), value)
    return value


def write_piece(emis_ref, bins_ref, at, packed, out_ref, ray_step):
    depth_cells, piece_rows, cols = emis_ref.shape[-3:]
    for r in range(0, piece_rows, ROWS):
        for col in range(0, cols, LANES):

            def cells(k):
                block = (*at, k, slice(r, r + ROWS), slice(col, col + LANES))
                return emis_ref[block], bins_ref[block]

            planes = block_partial(cells, packed, depth_cells, ray_step)
            for ch, plane in enumerate(planes):
                out_ref[ch, r : r + ROWS, col : col + LANES] = plane


def first_kernel(
    emis_hbm, bins_hbm, table_hbm, order_hbm, *refs, targets, ray_step, ready
):
    n = len(targets)
    out_refs = refs[: n - 1]
    emis_own, bins_own, packed_ref, order_ref = refs[n - 1 : n + 3]
    emis_ref, bins_ref, table_ref, sems, table_sem, order_sem = refs[n + 3 :]
    me = lax.axis_index("depth")
    piece_rows = emis_own.shape[1]
    table_copy = pltpu.make_async_copy(table_hbm, table_ref, table_sem)
    table_copy.start()
    copies = []
    for s in range(n):
        row = pl.multiple_of(lookup(targets[s], me) * piece_rows, piece_rows)
        src = pl.ds(row, piece_rows)
        bins_to = bins_ref.at[s] if s < n - 1 else bins_own
        emis_to = emis_ref.at[s] if s < n - 1 else emis_own
        pair = (
            pltpu.make_async_copy(bins_hbm.at[:, src, :], bins_to, sems.at[s, 0]),
            pltpu.make_async_copy(emis_hbm.at[:, src, :], emis_to, sems.at[s, 1]),
        )
        copies.append(pair)
        for copy in pair:
            copy.start()
    order_copy = pltpu.make_async_copy(order_hbm, order_ref, order_sem)
    order_copy.start()
    table_copy.wait()
    packed = load_table(table_ref, ROWS)
    for pair, chunks in enumerate(packed):
        for c, chunk in enumerate(chunks):
            packed_ref[pair, c] = chunk
    start = 0
    for count in ready:
        some = range(start, min(start + count, n - 1))
        for s in some:
            for copy in copies[s]:
                copy.wait()
        for s in some:
            write_piece(emis_ref, bins_ref, (s,), packed, out_refs[s], ray_step)
        start += count
    for copy in copies[n - 1]:
        copy.wait()
    order_copy.wait()


def own_kernel(emis_ref, bins_ref, packed_ref, out_ref, *, ray_step):
    pairs, chunks = packed_ref.shape[:2]
    packed = [[packed_ref[pair, c] for c in range(chunks)] for pair in range(pairs)]
    write_piece(emis_ref, bins_ref, (), packed, out_ref, ray_step)


def composite_kernel(order_ref, *refs, slots):
    me = lax.axis_index("depth")
    in_refs, out_ref = refs[:-1], refs[-1]
    n = len(in_refs)

    def pick(slot, ch):
        value = in_refs[0][ch]
        for s in range(1, n):
            value = jnp.where(slot == s, in_refs[s][ch], value)
        return value

    flat = [s for row in slots for s in row]
    color = [None] * 3
    through = None
    for k in range(n):
        slot = lookup(flat, me * n + order_ref[k])
        for ch in range(3):
            term = pick(slot, ch)
            if k:
                term = color[ch] + through * term
            color[ch] = term
        passed = pick(slot, 3)
        through = passed if through is None else through * passed
    for ch in range(3):
        out_ref[ch] = color[ch]
    out_ref[3] = 1.0 - through


def assemble_kernel(*refs, sources):
    me = lax.axis_index("depth")
    in_refs, out_ref, sems = refs[:-2], refs[-2], refs[-1]
    piece_rows = in_refs[0].shape[1]
    copies = []
    for s, in_ref in enumerate(in_refs):
        row = pl.multiple_of(lookup(sources[s], me) * piece_rows, piece_rows)
        copies.append(
            pltpu.make_async_copy(in_ref, out_ref.at[:, pl.ds(row, piece_rows), :], sems.at[s])
        )
    for copy in copies:
        copy.start()
    for copy in copies:
        copy.wait()


def exchange(pieces, targets):
    received = []
    for s, target in enumerate(targets):
        received.append(lax.ppermute(pieces[s], "depth", list(enumerate(target))))
    return received


def rounds(devices, order):
    if devices == 4:
        return [list(target) for target in order]
    return [[d ^ s for d in range(devices)] for s in range(1, devices)]


def inverse(target):
    return [target.index(d) for d in range(len(target))]


VMEM = pl.BlockSpec(memory_space=pltpu.VMEM)
SMEM = pl.BlockSpec(memory_space=pltpu.SMEM)
ANY = pl.BlockSpec(memory_space=pl.ANY)


def in_vmem(arrays):
    return [pltpu.with_memory_space_constraint(a, pltpu.VMEM) for a in arrays]


def by_exchange(emissivity, bin_index, color_table, brick_order, devices, ray_step):
    depth_cells, cols_x, cols_y = emissivity.shape
    piece_rows = cols_x // devices
    out_targets = rounds(devices, OUT_ORDER)
    back_targets = rounds(devices, BACK_ORDER)
    mine_target = list(range(devices))
    piece = pltpu.VMEM((4, piece_rows, cols_y), jnp.float32)
    cells = (depth_cells, piece_rows, cols_y)
    n = devices
    channels, bins = color_table.shape
    *pieces, emis_own, bins_own, packed, order = pl.pallas_call(
        functools.partial(
            first_kernel, targets=out_targets + [mine_target], ray_step=ray_step, ready=READY if devices == 4 else (1,) * n
        ),
        out_shape=[piece] * (n - 1)
        + [
            pltpu.VMEM(cells, emissivity.dtype),
            pltpu.VMEM(cells, bin_index.dtype),
            pltpu.VMEM((channels // 2, bins // LANES, ROWS, LANES), jnp.int32),
            pltpu.SMEM(brick_order.shape, brick_order.dtype),
        ],
        in_specs=[ANY] * 4,
        out_specs=[VMEM] * (n + 2) + [SMEM],
        scratch_shapes=[
            pltpu.VMEM((n - 1, *cells), emissivity.dtype),
            pltpu.VMEM((n - 1, *cells), bin_index.dtype),
            pltpu.VMEM(color_table.shape, color_table.dtype),
            pltpu.SemaphoreType.DMA((n, 2)),
            pltpu.SemaphoreType.DMA,
            pltpu.SemaphoreType.DMA,
        ],
        name="first",
    )(emissivity, bin_index, color_table, brick_order)
    own = pl.pallas_call(
        functools.partial(own_kernel, ray_step=ray_step),
        out_shape=piece,
        in_specs=[VMEM] * 3,
        out_specs=VMEM,
        name="own_piece",
    )(*in_vmem([emis_own, bins_own, packed]))
    received = exchange(pieces, out_targets)
    slots = [[None] * devices for _ in range(devices)]
    for s, target in enumerate([mine_target] + out_targets):
        for d, t in enumerate(target):
            slots[t][d] = s
    mine = pl.pallas_call(
        functools.partial(composite_kernel, slots=slots),
        out_shape=pltpu.VMEM((4, piece_rows, cols_y), jnp.float32),
        in_specs=[SMEM] + [VMEM] * devices,
        out_specs=VMEM,
        name="composite",
    )(pltpu.with_memory_space_constraint(order, pltpu.SMEM), *in_vmem([own] + received))
    tiles = [mine] + exchange([mine] * (devices - 1), back_targets)
    sources = [inverse(t) for t in [mine_target] + back_targets]
    return pl.pallas_call(
        functools.partial(assemble_kernel, sources=sources),
        out_shape=jax.ShapeDtypeStruct((4, cols_x, cols_y), jnp.float32),
        in_specs=[VMEM] * devices,
        out_specs=ANY,
        scratch_shapes=[pltpu.SemaphoreType.DMA((devices,))],
        name="assemble",
    )(*in_vmem(tiles))


def whole_partial_kernel(emis_ref, bins_ref, table_ref, out_ref, *, ray_step, rows):
    packed = load_table(table_ref, rows)
    depth_cells, cols_x, cols_y = emis_ref.shape

    def step(b, carry):
        row = pl.multiple_of(b * rows, rows)
        for col in range(0, cols_y, LANES):

            def cells(k):
                at = (k, pl.ds(row, rows), slice(col, col + LANES))
                return emis_ref[at], bins_ref[at]

            planes = block_partial(cells, packed, depth_cells, ray_step)
            for ch, plane in enumerate(planes):
                out_ref[ch, pl.ds(row, rows), col : col + LANES] = plane
        return carry

    lax.fori_loop(0, cols_x // rows, step, 0)


def by_collectives(emissivity, bin_index, color_table, brick_order, devices, ray_step):
    _, cols_x, cols_y = emissivity.shape
    partials = pl.pallas_call(
        functools.partial(whole_partial_kernel, ray_step=ray_step, rows=8),
        out_shape=jax.ShapeDtypeStruct((4, cols_x, cols_y), jnp.float32),
        in_specs=[VMEM, VMEM, VMEM],
        out_specs=VMEM,
        name="partial_whole",
    )(emissivity, bin_index, color_table)
    pieces = partials.reshape(4, devices, cols_x // devices, cols_y).transpose(1, 0, 2, 3)
    received = lax.all_to_all(pieces, "depth", split_axis=0, concat_axis=0, tiled=True)

    def advance(state, brick):
        color, through = state
        planes = lax.dynamic_index_in_dim(received, brick, 0, keepdims=False)
        return (color + through * planes[0:3], through * planes[3]), None

    start = (jnp.zeros_like(received[0, 0:3]), jnp.ones_like(received[0, 3]))
    (color, through), _ = lax.scan(advance, start, brick_order)
    mine = jnp.concatenate([color, (1.0 - through)[None]], 0)
    return lax.all_gather(mine, "depth", axis=1, tiled=True)


def on_device(emissivity, bin_index, color_table, brick_order):
    depth_cells, cols_x, _ = emissivity.shape
    devices = lax.axis_size("depth")
    ray_step = 2.0 / (depth_cells * devices)
    few = devices in (2, 4, 8) and cols_x % (ROWS * devices) == 0
    plan = by_exchange if few else by_collectives
    return plan(emissivity, bin_index, color_table, brick_order, devices, ray_step)


def solution(mesh):
    return jax.shard_map(
        on_device,
        mesh=mesh,
        in_specs=(P("depth", "imgx", "imgy"), P("depth", "imgx", "imgy"), P(), P()),
        out_specs=P(None, "imgx", "imgy"),
        check_vma=False,
    )
```

```python
import functools
import math

import jax
import jax.numpy as jnp
from jax import lax
from jax.experimental import pallas as pl
from jax.experimental.pallas import tpu as pltpu
from jax.sharding import PartitionSpec as P


LANES = 128
TABLE_STEPS = 4096.0
FIELD_BITS = 13
FIELD = 1 << FIELD_BITS
ROWS = 8
OUT_ORDER = ((1, 3, 0, 2), (3, 2, 1, 0), (2, 0, 3, 1))
BACK_ORDER = ((1, 2, 3, 0), (2, 3, 0, 1), (3, 0, 1, 2))
LANE_GATHER = lax.GatherDimensionNumbers(
    offset_dims=(),
    collapsed_slice_dims=(1,),
    start_index_map=(1,),
    operand_batching_dims=(0,),
    start_indices_batching_dims=(0,),
)


def lane_lookup(table, index):
    return lax.gather(
        table,
        index[..., None],
        LANE_GATHER,
        slice_sizes=(1, 1),
        mode=lax.GatherScatterMode.PROMISE_IN_BOUNDS,
    )


def load_table(table_ref, rows):
    channels, bins = table_ref.shape
    table = table_ref[...].astype(jnp.float32)
    steps = (table * TABLE_STEPS).astype(jnp.int32)
    packed = []
    for ch in range(0, channels, 2):
        row = steps[ch : ch + 1, :] * FIELD + steps[ch + 1 : ch + 2, :]
        packed.append(
            [jnp.broadcast_to(row[:, c : c + LANES], (rows, LANES)) for c in range(0, bins, LANES)]
        )
    return packed


def table_lookup(chunks, bins):
    if len(chunks) == 1:
        both = lane_lookup(chunks[0], bins)
    else:
        low = bins % LANES
        high = bins // LANES
        both = lane_lookup(chunks[0], low)
        for c in range(1, len(chunks)):
            both = jnp.where(high == c, lane_lookup(chunks[c], low), both)
    first = lax.shift_right_logical(both, FIELD_BITS)
    second = both & (FIELD - 1)
    return first.astype(jnp.float32), second.astype(jnp.float32)


def block_partial(cells, packed, depth_cells, ray_step):
    rate_scale = -ray_step * math.log2(math.e) / TABLE_STEPS
    color = [None] * 3
    depth_sum = None
    for k in range(depth_cells):
        bright, bins = cells(k)
        bright = bright.astype(jnp.float32)
        red, green = table_lookup(packed[0], bins)
        blue, absorb = table_lookup(packed[1], bins)
        rate = bright * absorb
        if k:
            bright = bright * jnp.exp2(depth_sum * rate_scale)
        depth_sum = rate if depth_sum is None else depth_sum + rate
        for ch, factor in enumerate((red, green, blue)):
            term = bright * factor
            color[ch] = term if color[ch] is None else color[ch] + term
    scale = ray_step / TABLE_STEPS
    return [c * scale for c in color] + [jnp.exp2(depth_sum * rate_scale)]


def lookup(table, me):
    value = jnp.int32(table[0])
    for d in range(1, len(table)):
        value = jnp.where(me == d, jnp.int32(table[d]), value)
    return value


def write_piece(emis_ref, bins_ref, at, packed, out_ref, ray_step):
    depth_cells, piece_rows, cols = emis_ref.shape[-3:]
    for r in range(0, piece_rows, ROWS):
        for col in range(0, cols, LANES):

            def cells(k):
                block = (*at, k, slice(r, r + ROWS), slice(col, col + LANES))
                return emis_ref[block], bins_ref[block]

            planes = block_partial(cells, packed, depth_cells, ray_step)
            for ch, plane in enumerate(planes):
                out_ref[ch, r : r + ROWS, col : col + LANES] = plane


def first_kernel(
    emis_hbm, bins_hbm, table_hbm, order_hbm,
    out_ref, second_ref, emis_rest, bins_rest, packed_ref, order_ref,
    emis_first, bins_first, table_ref, sems, table_sem, order_sem,
    *, targets, ray_step,
):
    me = lax.axis_index("depth")
    piece_rows = out_ref.shape[1]
    table_copy = pltpu.make_async_copy(table_hbm, table_ref, table_sem)
    table_copy.start()
    copies = []
    for s in range(len(targets)):
        row = pl.multiple_of(lookup(targets[s], me) * piece_rows, piece_rows)
        src = pl.ds(row, piece_rows)
        bins_to = bins_rest.at[s - 1] if s else bins_first
        emis_to = emis_rest.at[s - 1] if s else emis_first
        copies.append(pltpu.make_async_copy(bins_hbm.at[:, src, :], bins_to, sems.at[s, 0]))
        copies.append(pltpu.make_async_copy(emis_hbm.at[:, src, :], emis_to, sems.at[s, 1]))
        for copy in copies[-2:]:
            copy.start()
    order_copy = pltpu.make_async_copy(order_hbm, order_ref, order_sem)
    order_copy.start()
    table_copy.wait()
    packed = load_table(table_ref, ROWS)
    for pair, chunks in enumerate(packed):
        for c, chunk in enumerate(chunks):
            packed_ref[pair, c] = chunk
    for copy in copies[:2]:
        copy.wait()
    write_piece(emis_first, bins_first, (), packed, out_ref, ray_step)
    for copy in copies[2:4]:
        copy.wait()
    write_piece(emis_rest, bins_rest, (0,), packed, second_ref, ray_step)
    for copy in copies[4:]:
        copy.wait()
    order_copy.wait()


def later_kernel(emis_ref, bins_ref, packed_ref, *out_refs, start, ray_step):
    pairs, chunks = packed_ref.shape[:2]
    packed = [[packed_ref[pair, c] for c in range(chunks)] for pair in range(pairs)]
    for s, out_ref in enumerate(out_refs):
        write_piece(emis_ref, bins_ref, (start + s,), packed, out_ref, ray_step)


def composite_kernel(order_ref, *refs, slots):
    me = lax.axis_index("depth")
    in_refs, out_ref = refs[:-1], refs[-1]
    n = len(in_refs)

    def pick(slot, ch):
        value = in_refs[0][ch]
        for s in range(1, n):
            value = jnp.where(slot == s, in_refs[s][ch], value)
        return value

    flat = [s for row in slots for s in row]
    color = [None] * 3
    through = None
    for k in range(n):
        slot = lookup(flat, me * n + order_ref[k])
        for ch in range(3):
            term = pick(slot, ch)
            if k:
                term = color[ch] + through * term
            color[ch] = term
        passed = pick(slot, 3)
        through = passed if through is None else through * passed
    for ch in range(3):
        out_ref[ch] = color[ch]
    out_ref[3] = 1.0 - through


def assemble_kernel(*refs, sources):
    me = lax.axis_index("depth")
    in_refs, out_ref, sems = refs[:-2], refs[-2], refs[-1]
    piece_rows = in_refs[0].shape[1]
    copies = []
    for s, in_ref in enumerate(in_refs):
        row = pl.multiple_of(lookup(sources[s], me) * piece_rows, piece_rows)
        copies.append(
            pltpu.make_async_copy(in_ref, out_ref.at[:, pl.ds(row, piece_rows), :], sems.at[s])
        )
    for copy in copies:
        copy.start()
    for copy in copies:
        copy.wait()


def exchange(pieces, targets):
    received = []
    for s, target in enumerate(targets):
        received.append(lax.ppermute(pieces[s], "depth", list(enumerate(target))))
    return received


def rounds(devices, order):
    if devices == 4:
        return [list(target) for target in order]
    return [[d ^ s for d in range(devices)] for s in range(1, devices)]


def inverse(target):
    return [target.index(d) for d in range(len(target))]


VMEM = pl.BlockSpec(memory_space=pltpu.VMEM)
SMEM = pl.BlockSpec(memory_space=pltpu.SMEM)
ANY = pl.BlockSpec(memory_space=pl.ANY)


def in_vmem(arrays):
    return [pltpu.with_memory_space_constraint(a, pltpu.VMEM) for a in arrays]


def by_exchange(emissivity, bin_index, color_table, brick_order, devices, ray_step):
    depth_cells, cols_x, cols_y = emissivity.shape
    piece_rows = cols_x // devices
    out_targets = rounds(devices, OUT_ORDER)
    back_targets = rounds(devices, BACK_ORDER)
    mine_target = list(range(devices))
    piece = pltpu.VMEM((4, piece_rows, cols_y), jnp.float32)
    cells = (depth_cells, piece_rows, cols_y)
    n = devices
    channels, bins = color_table.shape
    first, second, emis_rest, bins_rest, packed, order = pl.pallas_call(
        functools.partial(first_kernel, targets=out_targets + [mine_target], ray_step=ray_step),
        out_shape=[
            piece,
            piece,
            pltpu.VMEM((n - 1, *cells), emissivity.dtype),
            pltpu.VMEM((n - 1, *cells), bin_index.dtype),
            pltpu.VMEM((channels // 2, bins // LANES, ROWS, LANES), jnp.int32),
            pltpu.SMEM(brick_order.shape, brick_order.dtype),
        ],
        in_specs=[ANY] * 4,
        out_specs=[VMEM] * 5 + [SMEM],
        scratch_shapes=[
            pltpu.VMEM(cells, emissivity.dtype),
            pltpu.VMEM(cells, bin_index.dtype),
            pltpu.VMEM(color_table.shape, color_table.dtype),
            pltpu.SemaphoreType.DMA((n, 2)),
            pltpu.SemaphoreType.DMA,
            pltpu.SemaphoreType.DMA,
        ],
        name="first",
    )(emissivity, bin_index, color_table, brick_order)

    def later(start, count):
        return pl.pallas_call(
            functools.partial(later_kernel, start=start, ray_step=ray_step),
            out_shape=[piece] * count,
            in_specs=[VMEM] * 3,
            out_specs=[VMEM] * count,
        )(*in_vmem([emis_rest, bins_rest, packed]))

    pieces = [first, second] + list(later(1, n - 3))
    (own,) = later(n - 2, 1)
    received = exchange(pieces, out_targets)
    slots = [[None] * devices for _ in range(devices)]
    for s, target in enumerate([mine_target] + out_targets):
        for d, t in enumerate(target):
            slots[t][d] = s
    mine = pl.pallas_call(
        functools.partial(composite_kernel, slots=slots),
        out_shape=pltpu.VMEM((4, piece_rows, cols_y), jnp.float32),
        in_specs=[SMEM] + [VMEM] * devices,
        out_specs=VMEM,
        name="composite",
    )(pltpu.with_memory_space_constraint(order, pltpu.SMEM), *in_vmem([own] + received))
    tiles = [mine] + exchange([mine] * (devices - 1), back_targets)
    sources = [inverse(t) for t in [mine_target] + back_targets]
    return pl.pallas_call(
        functools.partial(assemble_kernel, sources=sources),
        out_shape=jax.ShapeDtypeStruct((4, cols_x, cols_y), jnp.float32),
        in_specs=[VMEM] * devices,
        out_specs=ANY,
        scratch_shapes=[pltpu.SemaphoreType.DMA((devices,))],
        name="assemble",
    )(*in_vmem(tiles))


def whole_partial_kernel(emis_ref, bins_ref, table_ref, out_ref, *, ray_step, rows):
    packed = load_table(table_ref, rows)
    depth_cells, cols_x, cols_y = emis_ref.shape

    def step(b, carry):
        row = pl.multiple_of(b * rows, rows)
        for col in range(0, cols_y, LANES):

            def cells(k):
                at = (k, pl.ds(row, rows), slice(col, col + LANES))
                return emis_ref[at], bins_ref[at]

            planes = block_partial(cells, packed, depth_cells, ray_step)
            for ch, plane in enumerate(planes):
                out_ref[ch, pl.ds(row, rows), col : col + LANES] = plane
        return carry

    lax.fori_loop(0, cols_x // rows, step, 0)


def by_collectives(emissivity, bin_index, color_table, brick_order, devices, ray_step):
    _, cols_x, cols_y = emissivity.shape
    partials = pl.pallas_call(
        functools.partial(whole_partial_kernel, ray_step=ray_step, rows=8),
        out_shape=jax.ShapeDtypeStruct((4, cols_x, cols_y), jnp.float32),
        in_specs=[VMEM, VMEM, VMEM],
        out_specs=VMEM,
        name="partial_whole",
    )(emissivity, bin_index, color_table)
    pieces = partials.reshape(4, devices, cols_x // devices, cols_y).transpose(1, 0, 2, 3)
    received = lax.all_to_all(pieces, "depth", split_axis=0, concat_axis=0, tiled=True)

    def advance(state, brick):
        color, through = state
        planes = lax.dynamic_index_in_dim(received, brick, 0, keepdims=False)
        return (color + through * planes[0:3], through * planes[3]), None

    start = (jnp.zeros_like(received[0, 0:3]), jnp.ones_like(received[0, 3]))
    (color, through), _ = lax.scan(advance, start, brick_order)
    mine = jnp.concatenate([color, (1.0 - through)[None]], 0)
    return lax.all_gather(mine, "depth", axis=1, tiled=True)


def on_device(emissivity, bin_index, color_table, brick_order):
    depth_cells, cols_x, _ = emissivity.shape
    devices = lax.axis_size("depth")
    ray_step = 2.0 / (depth_cells * devices)
    few = devices in (4, 8) and cols_x % (ROWS * devices) == 0
    plan = by_exchange if few else by_collectives
    return plan(emissivity, bin_index, color_table, brick_order, devices, ray_step)


def solution(mesh):
    return jax.shard_map(
        on_device,
        mesh=mesh,
        in_specs=(P("depth", "imgx", "imgy"), P("depth", "imgx", "imgy"), P(), P()),
        out_specs=P(None, "imgx", "imgy"),
        check_vma=False,
    )
```

```python
import functools
import math

import jax
import jax.numpy as jnp
from jax import lax
from jax.experimental import pallas as pl
from jax.experimental.pallas import tpu as pltpu
from jax.sharding import PartitionSpec as P


LANES = 128
TABLE_STEPS = 4096.0
FIELD_BITS = 13
FIELD = 1 << FIELD_BITS
ROWS = 8
OUT_ORDER = ((1, 3, 0, 2), (3, 2, 1, 0), (2, 0, 3, 1))
BACK_ORDER = ((1, 2, 3, 0), (2, 3, 0, 1), (3, 0, 1, 2))
LANE_GATHER = lax.GatherDimensionNumbers(
    offset_dims=(),
    collapsed_slice_dims=(1,),
    start_index_map=(1,),
    operand_batching_dims=(0,),
    start_indices_batching_dims=(0,),
)


def lane_lookup(table, index):
    return lax.gather(
        table,
        index[..., None],
        LANE_GATHER,
        slice_sizes=(1, 1),
        mode=lax.GatherScatterMode.PROMISE_IN_BOUNDS,
    )


def load_table(table_ref, rows):
    channels, bins = table_ref.shape
    table = table_ref[...].astype(jnp.float32)
    steps = (table * TABLE_STEPS).astype(jnp.int32)
    packed = []
    for ch in range(0, channels, 2):
        row = steps[ch : ch + 1, :] * FIELD + steps[ch + 1 : ch + 2, :]
        packed.append(
            [jnp.broadcast_to(row[:, c : c + LANES], (rows, LANES)) for c in range(0, bins, LANES)]
        )
    return packed


def table_lookup(chunks, bins):
    if len(chunks) == 1:
        both = lane_lookup(chunks[0], bins)
    else:
        low = bins % LANES
        high = bins // LANES
        both = lane_lookup(chunks[0], low)
        for c in range(1, len(chunks)):
            both = jnp.where(high == c, lane_lookup(chunks[c], low), both)
    first = lax.shift_right_logical(both, FIELD_BITS)
    second = both & (FIELD - 1)
    return first.astype(jnp.float32), second.astype(jnp.float32)


def block_partial(cells, packed, depth_cells, ray_step):
    rate_scale = -ray_step * math.log2(math.e) / TABLE_STEPS
    color = [None] * 3
    depth_sum = None
    for k in range(depth_cells):
        bright, bins = cells(k)
        bright = bright.astype(jnp.float32)
        red, green = table_lookup(packed[0], bins)
        blue, absorb = table_lookup(packed[1], bins)
        rate = bright * absorb
        if k:
            bright = bright * jnp.exp2(depth_sum * rate_scale)
        depth_sum = rate if depth_sum is None else depth_sum + rate
        for ch, factor in enumerate((red, green, blue)):
            term = bright * factor
            color[ch] = term if color[ch] is None else color[ch] + term
    scale = ray_step / TABLE_STEPS
    return [c * scale for c in color] + [jnp.exp2(depth_sum * rate_scale)]


def lookup(table, me):
    value = jnp.int32(table[0])
    for d in range(1, len(table)):
        value = jnp.where(me == d, jnp.int32(table[d]), value)
    return value


def write_piece(emis_ref, bins_ref, at, packed, out_ref, ray_step):
    depth_cells, piece_rows, cols = emis_ref.shape[-3:]
    for r in range(0, piece_rows, ROWS):
        for col in range(0, cols, LANES):

            def cells(k):
                block = (*at, k, slice(r, r + ROWS), slice(col, col + LANES))
                return emis_ref[block], bins_ref[block]

            planes = block_partial(cells, packed, depth_cells, ray_step)
            for ch, plane in enumerate(planes):
                out_ref[ch, r : r + ROWS, col : col + LANES] = plane


def first_kernel(
    emis_hbm, bins_hbm, table_hbm, order_hbm,
    out_ref, second_ref, emis_rest, bins_rest, packed_ref, order_ref,
    emis_first, bins_first, table_ref, sems, table_sem, order_sem,
    *, targets, ray_step,
):
    me = lax.axis_index("depth")
    piece_rows = out_ref.shape[1]
    table_copy = pltpu.make_async_copy(table_hbm, table_ref, table_sem)
    table_copy.start()
    copies = []
    for s in range(len(targets)):
        row = pl.multiple_of(lookup(targets[s], me) * piece_rows, piece_rows)
        src = pl.ds(row, piece_rows)
        bins_to = bins_rest.at[s - 1] if s else bins_first
        emis_to = emis_rest.at[s - 1] if s else emis_first
        copies.append(pltpu.make_async_copy(bins_hbm.at[:, src, :], bins_to, sems.at[s, 0]))
        copies.append(pltpu.make_async_copy(emis_hbm.at[:, src, :], emis_to, sems.at[s, 1]))
        for copy in copies[-2:]:
            copy.start()
    order_copy = pltpu.make_async_copy(order_hbm, order_ref, order_sem)
    order_copy.start()
    table_copy.wait()
    packed = load_table(table_ref, ROWS)
    for pair, chunks in enumerate(packed):
        for c, chunk in enumerate(chunks):
            packed_ref[pair, c] = chunk
    for copy in copies[:2]:
        copy.wait()
    write_piece(emis_first, bins_first, (), packed, out_ref, ray_step)
    for copy in copies[2:4]:
        copy.wait()
    write_piece(emis_rest, bins_rest, (0,), packed, second_ref, ray_step)
    for copy in copies[4:]:
        copy.wait()
    order_copy.wait()


def later_kernel(emis_ref, bins_ref, packed_ref, *out_refs, start, ray_step):
    pairs, chunks = packed_ref.shape[:2]
    packed = [[packed_ref[pair, c] for c in range(chunks)] for pair in range(pairs)]
    for s, out_ref in enumerate(out_refs):
        write_piece(emis_ref, bins_ref, (start + s,), packed, out_ref, ray_step)


def composite_kernel(order_ref, *refs, slots):
    me = lax.axis_index("depth")
    in_refs, out_ref = refs[:-1], refs[-1]
    n = len(in_refs)

    def pick(slot, ch):
        value = in_refs[0][ch]
        for s in range(1, n):
            value = jnp.where(slot == s, in_refs[s][ch], value)
        return value

    flat = [s for row in slots for s in row]
    color = [None] * 3
    through = None
    for k in range(n):
        slot = lookup(flat, me * n + order_ref[k])
        for ch in range(3):
            term = pick(slot, ch)
            if k:
                term = color[ch] + through * term
            color[ch] = term
        passed = pick(slot, 3)
        through = passed if through is None else through * passed
    for ch in range(3):
        out_ref[ch] = color[ch]
    out_ref[3] = 1.0 - through


def assemble_kernel(*refs, sources):
    me = lax.axis_index("depth")
    in_refs, out_ref, sems = refs[: len(sources)], refs[-2], refs[-1]
    piece_rows = in_refs[0].shape[1]
    copies = []
    for s, in_ref in enumerate(in_refs):
        row = pl.multiple_of(lookup(sources[s], me) * piece_rows, piece_rows)
        copies.append(
            pltpu.make_async_copy(in_ref, out_ref.at[:, pl.ds(row, piece_rows), :], sems.at[s])
        )
    for copy in copies:
        copy.start()
    for copy in copies:
        copy.wait()


def exchange(pieces, targets):
    received = []
    for s, target in enumerate(targets):
        received.append(lax.ppermute(pieces[s], "depth", list(enumerate(target))))
    return received


def rounds(devices, order):
    if devices == 4:
        return [list(target) for target in order]
    return [[d ^ s for d in range(devices)] for s in range(1, devices)]


def inverse(target):
    return [target.index(d) for d in range(len(target))]


VMEM = pl.BlockSpec(memory_space=pltpu.VMEM)
SMEM = pl.BlockSpec(memory_space=pltpu.SMEM)
ANY = pl.BlockSpec(memory_space=pl.ANY)


def in_vmem(arrays):
    return [pltpu.with_memory_space_constraint(a, pltpu.VMEM) for a in arrays]


def by_exchange(emissivity, bin_index, color_table, brick_order, devices, ray_step):
    depth_cells, cols_x, cols_y = emissivity.shape
    piece_rows = cols_x // devices
    out_targets = rounds(devices, OUT_ORDER)
    back_targets = rounds(devices, BACK_ORDER)
    mine_target = list(range(devices))
    piece = pltpu.VMEM((4, piece_rows, cols_y), jnp.float32)
    cells = (depth_cells, piece_rows, cols_y)
    n = devices
    channels, bins = color_table.shape
    first, second, emis_rest, bins_rest, packed, order = pl.pallas_call(
        functools.partial(first_kernel, targets=out_targets + [mine_target], ray_step=ray_step),
        out_shape=[
            piece,
            piece,
            pltpu.VMEM((n - 1, *cells), emissivity.dtype),
            pltpu.VMEM((n - 1, *cells), bin_index.dtype),
            pltpu.VMEM((channels // 2, bins // LANES, ROWS, LANES), jnp.int32),
            pltpu.SMEM(brick_order.shape, brick_order.dtype),
        ],
        in_specs=[ANY] * 4,
        out_specs=[VMEM] * 5 + [SMEM],
        scratch_shapes=[
            pltpu.VMEM(cells, emissivity.dtype),
            pltpu.VMEM(cells, bin_index.dtype),
            pltpu.VMEM(color_table.shape, color_table.dtype),
            pltpu.SemaphoreType.DMA((n, 2)),
            pltpu.SemaphoreType.DMA,
            pltpu.SemaphoreType.DMA,
        ],
        name="first",
    )(emissivity, bin_index, color_table, brick_order)

    def later(start, count):
        return pl.pallas_call(
            functools.partial(later_kernel, start=start, ray_step=ray_step),
            out_shape=[piece] * count,
            in_specs=[VMEM] * 3,
            out_specs=[VMEM] * count,
        )(*in_vmem([emis_rest, bins_rest, packed]))

    pieces = [first, second] + list(later(1, n - 3))
    (own,) = later(n - 2, 1)
    received = exchange(pieces, out_targets)
    slots = [[None] * devices for _ in range(devices)]
    for s, target in enumerate([mine_target] + out_targets):
        for d, t in enumerate(target):
            slots[t][d] = s
    mine = pl.pallas_call(
        functools.partial(composite_kernel, slots=slots),
        out_shape=pltpu.VMEM((4, piece_rows, cols_y), jnp.float32),
        in_specs=[SMEM] + [VMEM] * devices,
        out_specs=VMEM,
        name="composite",
    )(pltpu.with_memory_space_constraint(order, pltpu.SMEM), *in_vmem([own] + received))
    tiles = [mine] + exchange([mine] * (devices - 1), back_targets)
    sources = [inverse(t) for t in [mine_target] + back_targets]
    early = n // 2

    def place(some, image):
        given = [] if image is None else [image]
        count = len(sources[some])
        return pl.pallas_call(
            functools.partial(assemble_kernel, sources=sources[some]),
            out_shape=jax.ShapeDtypeStruct((4, cols_x, cols_y), jnp.float32),
            in_specs=[VMEM] * count + [ANY] * len(given),
            out_specs=ANY,
            scratch_shapes=[pltpu.SemaphoreType.DMA((count,))],
            input_output_aliases={count: 0} if given else {},
        )(*in_vmem(tiles[some]), *given)

    image = place(slice(0, early), None)
    return place(slice(early, n), image)


def whole_partial_kernel(emis_ref, bins_ref, table_ref, out_ref, *, ray_step, rows):
    packed = load_table(table_ref, rows)
    depth_cells, cols_x, cols_y = emis_ref.shape

    def step(b, carry):
        row = pl.multiple_of(b * rows, rows)
        for col in range(0, cols_y, LANES):

            def cells(k):
                at = (k, pl.ds(row, rows), slice(col, col + LANES))
                return emis_ref[at], bins_ref[at]

            planes = block_partial(cells, packed, depth_cells, ray_step)
            for ch, plane in enumerate(planes):
                out_ref[ch, pl.ds(row, rows), col : col + LANES] = plane
        return carry

    lax.fori_loop(0, cols_x // rows, step, 0)


def by_collectives(emissivity, bin_index, color_table, brick_order, devices, ray_step):
    _, cols_x, cols_y = emissivity.shape
    partials = pl.pallas_call(
        functools.partial(whole_partial_kernel, ray_step=ray_step, rows=8),
        out_shape=jax.ShapeDtypeStruct((4, cols_x, cols_y), jnp.float32),
        in_specs=[VMEM, VMEM, VMEM],
        out_specs=VMEM,
        name="partial_whole",
    )(emissivity, bin_index, color_table)
    pieces = partials.reshape(4, devices, cols_x // devices, cols_y).transpose(1, 0, 2, 3)
    received = lax.all_to_all(pieces, "depth", split_axis=0, concat_axis=0, tiled=True)

    def advance(state, brick):
        color, through = state
        planes = lax.dynamic_index_in_dim(received, brick, 0, keepdims=False)
        return (color + through * planes[0:3], through * planes[3]), None

    start = (jnp.zeros_like(received[0, 0:3]), jnp.ones_like(received[0, 3]))
    (color, through), _ = lax.scan(advance, start, brick_order)
    mine = jnp.concatenate([color, (1.0 - through)[None]], 0)
    return lax.all_gather(mine, "depth", axis=1, tiled=True)


def on_device(emissivity, bin_index, color_table, brick_order):
    depth_cells, cols_x, _ = emissivity.shape
    devices = lax.axis_size("depth")
    ray_step = 2.0 / (depth_cells * devices)
    few = devices in (4, 8) and cols_x % (ROWS * devices) == 0
    plan = by_exchange if few else by_collectives
    return plan(emissivity, bin_index, color_table, brick_order, devices, ray_step)


def solution(mesh):
    return jax.shard_map(
        on_device,
        mesh=mesh,
        in_specs=(P("depth", "imgx", "imgy"), P("depth", "imgx", "imgy"), P(), P()),
        out_specs=P(None, "imgx", "imgy"),
        check_vma=False,
    )
```
